32 devices in a mesh: section: 4 (over z), seq: 4 (over y, x), head: 2 (over core).
Axes of the slice: x: 2, y: 2, z: 4, core: 2. Of those that a mesh axis runs over, the one named last changes fastest.
Arguments:
- text_hidden: bfloat16 [4096, 4096], P('seq'), may hold values from -600 to 600
- norm_gain: float32 [4096], replicated, may hold values from 0.1 to 1.9
- image_features: bfloat16 [8192, 1024], P('seq'), may hold values from -6 to 6
- query_weight: bfloat16 [4096, 4096], P(None, ('section', 'head')), may hold values from -30 to 30
- key_weight: bfloat16 [1024, 1024], P(None, ('section', 'head')), may hold values from -0.75 to 0.75
- value_weight: bfloat16 [1024, 1024], P(None, ('section', 'head')), may hold values from -0.1875 to 0.1875
- output_weight: bfloat16 [4096, 4096], P(('section', 'head')), may hold values from -0.125 to 0.125
- selected: int32 [32, 16], P('seq'), may hold values from 0 to 127, as said below
Outputs:
- attn_output: bfloat16 [4096, 4096], P('seq', ('section', 'head'))
The draws below stay inside these ranges and needn't reach their ends.
Inputs may be any that keep to these rules, and one draw needn't show every extreme that they name: `selected`: each row names 16 different image blocks. The tiles of one seq index together select at most 32 different blocks from the 32 blocks of any one seq index, and exactly 32 from some seq index.
All inputs are finite; a program needn't handle non-finite values.
Results may differ from the reference program's by a relative error of at most 0.0069.
The reference program's roundings to bfloat16 on the way (of `normed`, `queries`, `weights` and `attended`) count: a program that leaves them out, or rounds other values in their place, can miss the bound.
Values may be sent and summed in bfloat16 or wider, within the bound.
A program may use at most 128 MiB of HBM per device.

```python
import jax
import jax.numpy as jnp
from jax import lax

D = 4096
HEADS = 32
KV_HEADS = 8
HEAD_DIM = 128
ENC = 1024
TILE = 128
BLOCK = 64
TOPK = 16
BLOCKS_DEV = 32
TEXT = 4096
TILES = 32
BLOCKS = 128
IMAGE = 8192
CAP = 32
N_SEQ = 4


def draw_text_hidden(key, part):
    first_key = jax.random.fold_in(jax.random.fold_in(key, 11), 0)
    sample = jnp.clip(jax.random.normal(first_key, (TEXT, D), jnp.float32), -6.0, 6.0)
    return sample.astype(jnp.bfloat16)


def draw_query_weight(key, part):
    first_key = jax.random.fold_in(jax.random.fold_in(key, 23), 0)
    sample = jnp.clip(jax.random.normal(first_key, (D, HEADS * HEAD_DIM), jnp.float32), -6.0, 6.0) * D ** (-0.5)
    return sample.astype(jnp.bfloat16)


def pick_for_device(device_key):
    owner_key, local_key, start_key = jax.random.split(device_key, 3)
    owners = jax.random.permutation(owner_key, N_SEQ).astype(jnp.int32)
    local_keys = jax.random.split(local_key, N_SEQ)
    locals_all = jax.vmap(lambda one_key: jax.random.permutation(one_key, BLOCKS_DEV)[:CAP].astype(jnp.int32))(local_keys)
    union = (owners[:, None] * BLOCKS_DEV + locals_all).reshape(N_SEQ * CAP)
    tiles_dev = TILES // N_SEQ
    rotation = jax.random.randint(start_key, (), 0, N_SEQ).astype(jnp.int32) * CAP
    position = (rotation + jnp.arange(tiles_dev, dtype=jnp.int32)[:, None] * TOPK + jnp.arange(TOPK, dtype=jnp.int32)[None, :]) % (N_SEQ * CAP)
    return union[position]


def draw_selected(key, part):
    device_keys = jax.random.split(jax.random.fold_in(key, 37), N_SEQ)
    picked = jax.vmap(pick_for_device)(device_keys)
    return picked.reshape(TILES, TOPK).astype(jnp.int32)


def with_spikes(entries, stream_key, source, target, parts, factor):
    def block_of(axis_at):
        return (jnp.arange(entries.shape[axis_at]) // (entries.shape[axis_at] // parts)).reshape((-1,) + (1,) * (entries.ndim - 1 - axis_at))

    first = jax.random.permutation(stream_key, parts)[block_of(target)]
    other_side = (block_of(target) + parts // 2) % parts
    return jnp.where((block_of(source) == first) | (block_of(source) == other_side), factor * entries, entries)


def levels(rng, shape, cuts, low, high):
    def one(dim, parts):
        heights = jax.random.uniform(jax.random.fold_in(jax.random.fold_in(rng, 6), dim), (parts,), jnp.float32, low / len(cuts), high / len(cuts))
        return jnp.repeat(jnp.exp(heights), shape[dim] // parts).reshape((-1,) + (1,) * (len(shape) - dim - 1))

    level = one(*cuts[0])
    for cut in cuts[1:]:
        level = level * one(*cut)
    return level


def scatter_about(own_key, shape, scale, limit, cuts=(), kind=jnp.bfloat16):
    entries = jax.random.normal(own_key, shape, jnp.float32) * scale
    if len(cuts) > 0:
        entries = levels(own_key, shape, cuts, -0.22, 0.18) * entries
    return jnp.clip(entries, min=-limit, max=limit).astype(kind)


def bell_draw_with(rng, extent, width, reach, pieces, heavy, held_as=jnp.bfloat16):
    result = width * jax.random.normal(rng, extent, jnp.float32)
    if pieces:
        result = result * levels(rng, extent, pieces, -0.22, 0.18)
    return jnp.clip(with_spikes(result, jax.random.fold_in(rng, 3), *heavy), -reach, reach).astype(held_as)


def setup_inputs(seed: int = 0) -> dict:
    arg_keys = jax.random.split(jax.random.key(seed), 9)
    return {
        "text_hidden": draw_text_hidden(jax.random.fold_in(arg_keys[8], 71), 0),
        "norm_gain": jnp.clip(1.0 + 0.18 * jax.random.normal(arg_keys[1], (D,), jnp.float32), 0.1, 1.9),
        "image_features": scatter_about(arg_keys[2], (IMAGE, ENC), 1.0, 6.0, ((0, 4),)),
        "query_weight": draw_query_weight(jax.random.fold_in(arg_keys[8], 71), 0),
        "key_weight": scatter_about(arg_keys[4], (ENC, KV_HEADS * HEAD_DIM), (ENC // 16) ** -0.5, 0.75, ((1, 8),)),
        "value_weight": scatter_about(arg_keys[5], (ENC, KV_HEADS * HEAD_DIM), ENC ** -0.5, 0.1875, ((1, 8),)),
        "output_weight": bell_draw_with(arg_keys[6], (HEADS * HEAD_DIM, D), (HEADS * HEAD_DIM) ** -0.5, 0.125, ((0, 8),), (0, 1, 8, 2.0)),
        "selected": draw_selected(jax.random.fold_in(arg_keys[8], 71), 0),
    }


EPSILON = 1e-05

def reference(text_hidden, norm_gain, image_features, query_weight, key_weight, value_weight, output_weight, selected):
    as_float = text_hidden.astype(jnp.float32)
    inverse = lax.rsqrt(lax.optimization_barrier(jnp.mean(as_float * as_float, axis=-1, keepdims=True)) + EPSILON)
    normed = (as_float * inverse * norm_gain).astype(jnp.bfloat16)
    queries = jnp.dot(normed, query_weight, preferred_element_type=jnp.float32).astype(jnp.bfloat16)
    key_rows = jnp.dot(image_features, key_weight, preferred_element_type=jnp.float32).astype(jnp.bfloat16)
    value_rows = jnp.dot(image_features, value_weight, preferred_element_type=jnp.float32).astype(jnp.bfloat16)
    group_size = HEADS // KV_HEADS
    key_blocks = key_rows.reshape(BLOCKS, BLOCK, KV_HEADS, HEAD_DIM)
    value_blocks = value_rows.reshape(BLOCKS, BLOCK, KV_HEADS, HEAD_DIM)
    query_tiles = queries.reshape(TILES, TILE, KV_HEADS, group_size, HEAD_DIM)

    def one_tile(tile_input):
        tile_queries, picked = tile_input
        tile_keys = key_blocks[picked].reshape(TOPK * BLOCK, KV_HEADS, HEAD_DIM).astype(jnp.float32)
        tile_values = value_blocks[picked].reshape(TOPK * BLOCK, KV_HEADS, HEAD_DIM).astype(jnp.float32)
        scores = jnp.einsum('tkgd,skd->kgts', tile_queries.astype(jnp.float32), tile_keys) * HEAD_DIM ** (-0.5)
        largest = lax.optimization_barrier(jnp.max(scores, axis=-1, keepdims=True))
        exponent = jnp.exp(scores - largest)
        weights = (exponent / lax.optimization_barrier(jnp.sum(exponent, axis=-1, keepdims=True))).astype(jnp.bfloat16)
        attended = jnp.einsum('kgts,skd->tkgd', weights.astype(jnp.float32), tile_values)
        return attended.astype(jnp.bfloat16)
    attended = lax.map(one_tile, (query_tiles, selected))
    attended = attended.reshape(TILES * TILE, HEADS * HEAD_DIM)
    return jnp.dot(attended, output_weight, preferred_element_type=jnp.float32).astype(jnp.bfloat16)
```

```python
import functools

import jax
import jax.numpy as jnp
from jax import lax
from jax.experimental import pallas as pl
from jax.experimental.pallas import tpu as pltpu
from jax.sharding import PartitionSpec as P

HEAD_DIM = 128
TILE = 128
BLOCK = 64
EPSILON = 1e-05
CHUNKS = 4
PART_LAG = 4
OUT_LAG = 2
MESH = pl.DeviceIdType.MESH


def kernel(
    sizes,
    text_hbm,
    gain_ref,
    image_hbm,
    wq_hbm,
    wk_hbm,
    wv_hbm,
    wo_hbm,
    sel_ref,
    out_ref,
    text,
    image,
    wq,
    wkv,
    wo_all,
    part_out,
    part_in,
    k_all,
    v_all,
    q_all,
    k_sel,
    v_sel,
    att,
    text_sem,
    image_sem,
    weight_sem,
    kv_send,
    kv_recv,
    fwd_send,
    fwd_recv,
    wo_local,
    wo_send,
    wo_recv,
    z_send,
    z_recv,
    g_send,
    g_recv,
    gf_send,
    gf_recv,
    go_sem,
    a_send,
    a_core,
    r_pair,
    r_core,
    p_send,
    p_recv,
):
    n_sec, n_seq, n_head = sizes
    sec = lax.axis_index("section")
    seq = lax.axis_index("seq")
    head = lax.axis_index("head")
    tiles = q_all.shape[0]
    qk_rows = q_all.shape[1]
    heads = qk_rows // TILE
    width = k_all.shape[-1]
    local_kv = width // HEAD_DIM
    group = heads // local_kv
    topk = sel_ref.shape[1]
    rows_img = image.shape[0]
    blocks_dev = rows_img // BLOCK
    chunk_blocks = blocks_dev // CHUNKS
    chunk_rows = chunk_blocks * BLOCK
    out_cols = out_ref.shape[1]
    text_step = text_sem.shape[0]
    text_rows = text.shape[0] // text_step

    other = 1 - head
    buddy = lax.rem(sec + n_sec // 2, n_sec)
    far = sec + 1 - 2 * lax.rem(sec, 2)
    buddy_far = buddy + 1 - 2 * lax.rem(buddy, 2)
    first = head == 0

    def at(s, h):
        return {"section": s, "seq": seq, "head": h}

    def at_seq(q):
        return {"section": sec, "seq": q, "head": head}

    def remote(src, dst, send, recv, device):
        return pltpu.make_async_remote_copy(
            src_ref=src, dst_ref=dst, send_sem=send, recv_sem=recv, device_id=device, device_id_type=MESH
        )

    weight_loads = [
        pltpu.make_async_copy(wk_hbm, wkv.at[:, pl.ds(0, width)], weight_sem.at[0]),
        pltpu.make_async_copy(wv_hbm, wkv.at[:, pl.ds(width, width)], weight_sem.at[1]),
        pltpu.make_async_copy(wq_hbm, wq, weight_sem.at[2]),
    ]
    image_loads = [
        pltpu.make_async_copy(
            image_hbm.at[pl.ds(c * chunk_rows, chunk_rows)],
            image.at[pl.ds(c * chunk_rows, chunk_rows)],
            image_sem.at[c],
        )
        for c in range(CHUNKS)
    ]
    text_loads = [
        pltpu.make_async_copy(
            text_hbm.at[pl.ds(c * text_rows, text_rows)],
            text.at[pl.ds(c * text_rows, text_rows)],
            text_sem.at[c],
        )
        for c in range(text_step)
    ]
    weight_loads[0].start()
    weight_loads[1].start()
    for load in image_loads:
        load.start()
    weight_loads[2].start()
    for load in text_loads:
        load.start()

    barrier = pltpu.get_barrier_semaphore()
    for d in range(1, n_seq):
        pl.semaphore_signal(barrier, inc=1, device_id=at_seq(lax.rem(seq + d, n_seq)), device_id_type=MESH)
    for d in range(n_sec):
        for e in range(n_head):
            if d or e:
                pl.semaphore_signal(
                    barrier,
                    inc=1,
                    device_id=at(lax.rem(sec + d, n_sec), lax.rem(head + e, n_head)),
                    device_id_type=MESH,
                )
    pl.semaphore_wait(barrier, n_seq - 1 + n_sec * n_head - 1)

    def slot(flag, h):
        return flag * n_head + h

    def wo_cols(s, h):
        return pl.ds(pl.multiple_of((s * n_head + h) * out_cols, out_cols), out_cols)

    wo_own = [
        pltpu.make_async_copy(
            wo_hbm.at[:, wo_cols((sec, far)[side], head)], wo_all.at[side, slot(0, head)], wo_local.at[side]
        )
        for side in range(2)
    ]
    wo_near = [
        remote(
            wo_hbm.at[:, wo_cols((sec, far)[side], other)],
            wo_all.at[side, slot(0, head)],
            wo_send.at[side],
            wo_recv.at[side],
            at(sec, other),
        )
        for side in (1, 0)
    ]
    piece_rows = wo_hbm.shape[0] // n_seq

    def piece_at(side, h, owner):
        return wo_all.at[side, slot(1, h), pl.ds(pl.multiple_of(owner * piece_rows, piece_rows), piece_rows)]

    wo_far = [
        remote(
            wo_hbm.at[
                pl.ds(pl.multiple_of(seq * piece_rows, piece_rows), piece_rows), wo_cols((buddy, buddy_far)[side], h)
            ],
            piece_at(side, head, seq),
            z_send.at[side, i],
            z_recv.at[side, i],
            at(buddy, h),
        )
        for side in (1, 0)
        for i, h in enumerate((head, other))
    ]
    for copy in wo_far + wo_own + wo_near:
        copy.start()

    weight_loads[0].wait()
    weight_loads[1].wait()

    def chunk_at(ref, owner, c):
        return ref.at[pl.ds(owner * blocks_dev + c * chunk_blocks, chunk_blocks)]

    ring = n_seq == 4
    if ring:
        sx, sy = lax.rem(seq, 2), seq // 2
        beside = sy * 2 + (1 - sx)
        across = (1 - sy) * 2 + sx
        peers = [beside, across]
    else:
        peers = [lax.rem(seq + d, n_seq) for d in range(1, n_seq)]

    def kv_copy(kind, peer_at, c):
        ref = (k_all, v_all)[kind]
        return remote(
            chunk_at(ref, seq, c),
            chunk_at(ref, seq, c),
            kv_send.at[kind, peer_at, c],
            kv_recv.at[kind, peer_at, c],
            at_seq(peers[peer_at]),
        )

    def kv_start_early(c):
        if ring:
            kv_copy(0, 1, c).start()
            kv_copy(1, 0, c).start()
        else:
            for p in range(len(peers)):
                kv_copy(0, p, c).start()
                kv_copy(1, p, c).start()

    def kv_start_late():
        if ring:
            for c in range(CHUNKS):
                kv_copy(1, 1, c).start()
                kv_copy(0, 0, c).start()

    for c in range(CHUNKS):
        image_loads[c].wait()
        both = jnp.dot(
            image[c * chunk_rows : (c + 1) * chunk_rows, :], wkv[...], preferred_element_type=jnp.float32
        ).astype(jnp.bfloat16)
        base = pl.ds(seq * blocks_dev + c * chunk_blocks, chunk_blocks)
        k_all[base] = both[:, :width].reshape(chunk_blocks, BLOCK, width)
        v_all[base] = both[:, width:].reshape(chunk_blocks, BLOCK, width)

        @pl.when(first)
        def _():
            kv_start_early(c)

    @pl.when(first)
    def _():
        kv_start_late()

    weight_loads[2].wait()
    for load in text_loads:
        load.wait()

    def query_step(i, carry):
        part = pl.ds(pl.multiple_of(i * text_rows, text_rows), text_rows)
        as_float = text[part, :].astype(jnp.float32)
        inverse = lax.rsqrt(jnp.mean(as_float * as_float, axis=-1, keepdims=True) + EPSILON)
        normed = (as_float * inverse * gain_ref[...]).astype(jnp.bfloat16)
        queries = jnp.dot(normed, wq[...], preferred_element_type=jnp.float32).astype(jnp.bfloat16)
        for u in range(text_rows // TILE):
            for h in range(heads):
                q_all[i * (text_rows // TILE) + u, h * TILE : (h + 1) * TILE, :] = queries[
                    u * TILE : (u + 1) * TILE, h * HEAD_DIM : (h + 1) * HEAD_DIM
                ]
        return carry

    lax.fori_loop(0, text_step, query_step, 0)

    def kv_arrival(kind, peer_at, c):
        ref = (k_all, v_all)[kind]
        back = peer_at if ring else len(peers) - 1 - peer_at
        there = chunk_at(ref, peers[back], c)
        return remote(there, there, kv_send.at[kind, peer_at, c], kv_recv.at[kind, peer_at, c], at_seq(peers[peer_at]))

    def kv_forward(kind, c):
        ref = (k_all, v_all)[kind]
        came, goes = ((across, beside), (beside, across))[kind]
        there = chunk_at(ref, came, c)
        return remote(there, there, fwd_send.at[kind, c], fwd_recv.at[kind, c], at_seq(goes))

    def kv_forwarded(kind, c):
        ref = (k_all, v_all)[kind]
        there = chunk_at(ref, 3 - seq, c)
        return remote(there, there, fwd_send.at[kind, c], fwd_recv.at[kind, c], at_seq(seq))

    @pl.when(jnp.logical_not(first))
    def _():
        pl.semaphore_wait(go_sem, 1)
        for c in range(CHUNKS):
            kv_start_early(c)
        kv_start_late()

    def kv_done(c):
        if ring:
            kv_arrival(0, 0, c).wait_recv()
            kv_arrival(1, 1, c).wait_recv()
            kv_forwarded(0, c).wait_recv()
            kv_forwarded(1, c).wait_recv()
        else:
            for p in range(len(peers)):
                kv_arrival(0, p, c).wait_recv()
                kv_arrival(1, p, c).wait_recv()

    def g_copy(side, i, peer_at):
        piece = piece_at(side, (head, other)[i], seq)
        return remote(piece, piece, g_send.at[side, i, peer_at], g_recv.at[side, i, peer_at], at_seq(peers[peer_at]))

    def g_arrival(side, i, peer_at):
        back = peer_at if ring else len(peers) - 1 - peer_at
        there = piece_at(side, (head, other)[i], peers[back])
        return remote(there, there, g_send.at[side, i, peer_at], g_recv.at[side, i, peer_at], at_seq(peers[peer_at]))

    def g_forward(side, i):
        came, goes = ((across, beside), (beside, across))[i]
        there = piece_at(side, (head, other)[i], came)
        return remote(there, there, gf_send.at[side, i], gf_recv.at[side, i], at_seq(goes))

    def g_forwarded(side, i):
        there = piece_at(side, (head, other)[i], 3 - seq)
        return remote(there, there, gf_send.at[side, i], gf_recv.at[side, i], at_seq(peers[0]))

    def spread_wo(side):
        for i in range(2):
            there = piece_at(side, (head, other)[i], seq)
            remote(there, there, z_send.at[side, i], z_recv.at[side, i], at(buddy, head)).wait_recv()
        for i in range(2):
            if ring:
                g_copy(side, i, 1 - i).start()
            else:
                for p in range(len(peers)):
                    g_copy(side, i, p).start()
        if ring:
            for i in range(2):
                g_copy(side, i, i).start()

    def forward_wo(side):
        if ring:
            for i in range(2):
                g_arrival(side, i, 1 - i).wait_recv()
                g_forward(side, i).start()

    def wo_arrived(side):
        wo_own[side].wait()
        there = wo_all.at[side, slot(0, other)]
        remote(there, there, wo_send.at[side], wo_recv.at[side], at(sec, other)).wait_recv()
        for i in range(2):
            if ring:
                g_arrival(side, i, i).wait_recv()
                g_forwarded(side, i).wait_recv()
            else:
                for p in range(len(peers)):
                    g_arrival(side, i, p).wait_recv()

    if ring:
        for c in range(CHUNKS):
            kv_arrival(0, 1, c).wait_recv()
            kv_forward(0, c).start()
            kv_arrival(1, 0, c).wait_recv()
            kv_forward(1, c).start()

    @pl.when(jnp.logical_not(first))
    def _():
        spread_wo(1)
        spread_wo(0)

    for c in range(CHUNKS - 1):
        kv_done(c)

    @pl.when(first)
    def _():
        pl.semaphore_signal(go_sem, inc=1, device_id=at(sec, other), device_id_type=MESH)

    kv_done(CHUNKS - 1)

    def own_copies(t):
        tile = att.at[slot(0, head), t]
        return (
            remote(tile, att.at[slot(1, head), t], a_send.at[0, t], r_pair.at[t], at(buddy, head)),
            remote(tile, tile, a_send.at[1, t], r_core.at[0, t], at(sec, other)),
        )

    def pair_forward(t):
        tile = att.at[slot(1, head), t]
        return remote(tile, tile, a_core.at[t], r_core.at[1, t], at(sec, other))

    def part_copy(t):
        return remote(part_out.at[t], part_in.at[t], p_send.at[t], p_recv.at[t], at(far, head))

    def attend(t):
        for j in range(topk):
            block = sel_ref[t, j]
            k_sel[j * BLOCK : (j + 1) * BLOCK, :] = k_all[block]
            v_sel[j * BLOCK : (j + 1) * BLOCK, :] = v_all[block]
        for h in range(heads):
            kv = (h // group) * HEAD_DIM
            scores = lax.dot_general(
                q_all[t, h * TILE : (h + 1) * TILE, :],
                k_sel[:, kv : kv + HEAD_DIM],
                (((1,), (1,)), ((), ())),
                preferred_element_type=jnp.float32,
            ) * HEAD_DIM ** (-0.5)
            exponent = jnp.exp(scores - jnp.max(scores, axis=-1, keepdims=True))
            weights = (exponent * (1.0 / jnp.sum(exponent, axis=-1, keepdims=True))).astype(jnp.bfloat16)
            att[slot(0, head), t, :, h * HEAD_DIM : (h + 1) * HEAD_DIM] = jnp.dot(
                weights, v_sel[:, kv : kv + HEAD_DIM], preferred_element_type=jnp.float32
            ).astype(jnp.bfloat16)

    def product(side, t):
        total = None
        for i in range(2 * n_head):
            term = jnp.dot(att[i, t], wo_all[side, i], preferred_element_type=jnp.float32)
            total = term if total is None else total + term
        return total

    lag_part = jnp.where(first, tiles + 1, PART_LAG)
    lag_out = jnp.where(first, tiles + 1 + OUT_LAG, tiles + OUT_LAG)
    at_spread = tiles - 1
    at_forward = jnp.where(first, tiles, PART_LAG - 1)

    def step(s, carry):
        @pl.when(s < tiles)
        def _():
            attend(s)
            for copy in own_copies(s):
                copy.start()

        @pl.when((s >= 1) & (s < tiles + 1))
        def _():
            t = s - 1
            there = att.at[slot(1, head), t]
            remote(there, there, a_send.at[0, t], r_pair.at[t], at(buddy, head)).wait_recv()
            pair_forward(t).start()

        @pl.when(first & (s == at_spread))
        def _():
            spread_wo(1)
            spread_wo(0)

        @pl.when(s == at_forward)
        def _():
            forward_wo(1)

        @pl.when(s == at_forward + 1)
        def _():
            wo_arrived(1)
            forward_wo(0)

        @pl.when((s >= lag_part) & (s < tiles + lag_part))
        def _():
            t = s - lag_part
            for flag in range(2):
                there = att.at[slot(flag, other), t]
                remote(there, there, a_send.at[1, t], r_core.at[flag, t], at(sec, other)).wait_recv()
            part_out[t] = product(1, t).astype(jnp.bfloat16)
            part_copy(t).start()

        @pl.when(s == lag_out)
        def _():
            wo_arrived(0)

        @pl.when((s >= lag_out) & (s < tiles + lag_out))
        def _():
            t = s - lag_out
            own = product(0, t)
            part_copy(t).wait_recv()
            out_ref[pl.ds(pl.multiple_of(t * TILE, TILE), TILE), :] = (own + part_in[t].astype(jnp.float32)).astype(
                out_ref.dtype
            )

        return carry

    lax.fori_loop(0, 2 * tiles + 1 + OUT_LAG, step, 0)

    for copy in wo_near + wo_far:
        copy.wait_send()
    for side in range(2):
        for i in range(2):
            for p in range(len(peers)):
                g_copy(side, i, p).wait_send()
            if ring:
                g_forward(side, i).wait_send()
    for c in range(CHUNKS):
        for kind in range(2):
            for p in range(len(peers)):
                kv_copy(kind, p, c).wait_send()
            if ring:
                kv_forward(kind, c).wait_send()

    def drain(t, carry):
        for copy in own_copies(t) + (pair_forward(t), part_copy(t)):
            copy.wait_send()
        return carry

    lax.fori_loop(0, tiles, drain, 0)


def solution(mesh):
    n_sec, n_seq, n_head = mesh.shape["section"], mesh.shape["seq"], mesh.shape["head"]

    def shards(text, gain, image, wq, wk, wv, wo, selected):
        rows, depth = text.shape
        tiles = rows // TILE
        cols_q = wq.shape[1]
        width = wk.shape[1]
        group = n_sec * n_head
        out_cols = wo.shape[1] // group
        blocks = image.shape[0] // BLOCK * n_seq
        keys = selected.shape[1] * BLOCK
        text_step = max(1, rows // (2 * TILE))
        peers = 2 if n_seq == 4 else n_seq - 1
        bf16 = jnp.bfloat16
        dma = pltpu.SemaphoreType.DMA
        hbm = pl.BlockSpec(memory_space=pl.ANY)
        vmem = pl.BlockSpec(memory_space=pltpu.VMEM)
        return pl.pallas_call(
            functools.partial(kernel, (n_sec, n_seq, n_head)),
            out_shape=jax.ShapeDtypeStruct((rows, out_cols), bf16),
            in_specs=[hbm, vmem, hbm, hbm, hbm, hbm, hbm, pl.BlockSpec(memory_space=pltpu.SMEM)],
            out_specs=vmem,
            scratch_shapes=[
                pltpu.VMEM(text.shape, bf16),
                pltpu.VMEM(image.shape, bf16),
                pltpu.VMEM(wq.shape, bf16),
                pltpu.VMEM((wk.shape[0], 2 * width), bf16),
                pltpu.VMEM((2, 2 * n_head, wo.shape[0], out_cols), bf16),
                pltpu.VMEM((tiles, TILE, out_cols), bf16),
                pltpu.VMEM((tiles, TILE, out_cols), bf16),
                pltpu.VMEM((blocks, BLOCK, width), bf16),
                pltpu.VMEM((blocks, BLOCK, width), bf16),
                pltpu.VMEM((tiles, cols_q // HEAD_DIM * TILE, HEAD_DIM), bf16),
                pltpu.VMEM((keys, width), bf16),
                pltpu.VMEM((keys, width), bf16),
                pltpu.VMEM((2 * n_head, tiles, TILE, cols_q), bf16),
                dma((text_step,)),
                dma((CHUNKS,)),
                dma((3,)),
                dma((2, peers, CHUNKS)),
                dma((2, peers, CHUNKS)),
                dma((2, CHUNKS)),
                dma((2, CHUNKS)),
                dma((2,)),
                dma((2,)),
                dma((2,)),
                dma((2, 2)),
                dma((2, 2)),
                dma((2, 2, peers)),
                dma((2, 2, peers)),
                dma((2, 2)),
                dma((2, 2)),
                pltpu.SemaphoreType.REGULAR,
                dma((2, tiles)),
                dma((tiles,)),
                dma((tiles,)),
                dma((2, tiles)),
                dma((tiles,)),
                dma((tiles,)),
            ],
            compiler_params=pltpu.CompilerParams(
                collective_id=0, has_side_effects=True, vmem_limit_bytes=60 * 1024 * 1024
            ),
        )(text, gain.reshape(1, depth), image, wq, wk, wv, wo, selected)

    in_specs = (
        P("seq", None),
        P(),
        P("seq", None),
        P(None, ("section", "head")),
        P(None, ("section", "head")),
        P(None, ("section", "head")),
        P(("section", "head"), None),
        P("seq", None),
    )
    out_specs = P("seq", ("section", "head"))
    return jax.shard_map(shards, mesh=mesh, in_specs=in_specs, out_specs=out_specs, check_vma=False)
```

```python
import functools

import jax
import jax.numpy as jnp
from jax import lax
from jax.experimental import pallas as pl
from jax.experimental.pallas import tpu as pltpu
from jax.sharding import PartitionSpec as P

HEAD_DIM = 128
TILE = 128
BLOCK = 64
EPSILON = 1e-05
CHUNKS = 4
MESH = pl.DeviceIdType.MESH


def kernel(
    sizes,
    text_hbm,
    gain_ref,
    image_hbm,
    wq_hbm,
    wk_hbm,
    wv_hbm,
    wo_hbm,
    sel_ref,
    out_ref,
    text,
    image,
    wq,
    wkv,
    wo_all,
    part_out,
    part_in,
    k_all,
    v_all,
    q_all,
    k_sel,
    v_sel,
    att,
    text_sem,
    image_sem,
    weight_sem,
    kv_send,
    kv_recv,
    fwd_send,
    fwd_recv,
    wo_local,
    wo_send,
    wo_recv,
    z_send,
    z_recv,
    g_send,
    g_recv,
    gf_send,
    gf_recv,
    go_sem,
    a_send,
    a_core,
    r_pair,
    r_core,
    p_send,
    p_recv,
    f_send,
    f_recv,
):
    n_sec, n_seq, n_head = sizes
    sec = lax.axis_index("section")
    seq = lax.axis_index("seq")
    head = lax.axis_index("head")
    tiles = q_all.shape[0]
    qk_rows = q_all.shape[1]
    heads = qk_rows // TILE
    width = k_all.shape[-1]
    local_kv = width // HEAD_DIM
    group = heads // local_kv
    topk = sel_ref.shape[1]
    rows_img = image.shape[0]
    blocks_dev = rows_img // BLOCK
    chunk_blocks = blocks_dev // CHUNKS
    chunk_rows = chunk_blocks * BLOCK
    out_cols = out_ref.shape[1]
    text_step = text_sem.shape[0]
    text_rows = text.shape[0] // text_step

    other = 1 - head
    buddy = lax.rem(sec + n_sec // 2, n_sec)
    far = sec + 1 - 2 * lax.rem(sec, 2)
    buddy_far = buddy + 1 - 2 * lax.rem(buddy, 2)
    first = head == 0
    mine, theirs = jnp.where(first, far, sec), jnp.where(first, sec, far)
    mine_there, theirs_there = jnp.where(first, buddy_far, buddy), jnp.where(first, buddy, buddy_far)

    def at(s, h):
        return {"section": s, "seq": seq, "head": h}

    def at_seq(q):
        return {"section": sec, "seq": q, "head": head}

    def remote(src, dst, send, recv, device):
        return pltpu.make_async_remote_copy(
            src_ref=src, dst_ref=dst, send_sem=send, recv_sem=recv, device_id=device, device_id_type=MESH
        )

    weight_loads = [
        pltpu.make_async_copy(wk_hbm, wkv.at[:, pl.ds(0, width)], weight_sem.at[0]),
        pltpu.make_async_copy(wv_hbm, wkv.at[:, pl.ds(width, width)], weight_sem.at[1]),
        pltpu.make_async_copy(wq_hbm, wq, weight_sem.at[2]),
    ]
    image_loads = [
        pltpu.make_async_copy(
            image_hbm.at[pl.ds(c * chunk_rows, chunk_rows)],
            image.at[pl.ds(c * chunk_rows, chunk_rows)],
            image_sem.at[c],
        )
        for c in range(CHUNKS)
    ]
    text_loads = [
        pltpu.make_async_copy(
            text_hbm.at[pl.ds(c * text_rows, text_rows)],
            text.at[pl.ds(c * text_rows, text_rows)],
            text_sem.at[c],
        )
        for c in range(text_step)
    ]
    weight_loads[0].start()
    weight_loads[1].start()
    for load in image_loads:
        load.start()

    barrier = pltpu.get_barrier_semaphore()
    for d in range(1, n_seq):
        pl.semaphore_signal(barrier, inc=1, device_id=at_seq(lax.rem(seq + d, n_seq)), device_id_type=MESH)
    for d in range(n_sec):
        for e in range(n_head):
            if d or e:
                pl.semaphore_signal(
                    barrier,
                    inc=1,
                    device_id=at(lax.rem(sec + d, n_sec), lax.rem(head + e, n_head)),
                    device_id_type=MESH,
                )
    pl.semaphore_wait(barrier, n_seq - 1 + n_sec * n_head - 1)

    def slot(flag, h):
        return flag * n_head + h

    def wo_cols(s, h):
        return pl.ds(pl.multiple_of((s * n_head + h) * out_cols, out_cols), out_cols)

    wo_own = [
        pltpu.make_async_copy(
            wo_hbm.at[:, wo_cols(mine, side)], wo_all.at[side, slot(0, head)], wo_local.at[side]
        )
        for side in range(2)
    ]
    wo_near = [
        remote(
            wo_hbm.at[:, wo_cols(theirs, side)],
            wo_all.at[side, slot(0, head)],
            wo_send.at[side],
            wo_recv.at[side],
            at(sec, other),
        )
        for side in range(2)
    ]
    piece_rows = wo_hbm.shape[0] // n_seq

    def piece_at(side, h, owner):
        return wo_all.at[side, slot(1, h), pl.ds(pl.multiple_of(owner * piece_rows, piece_rows), piece_rows)]

    wo_far = [
        remote(
            wo_hbm.at[
                pl.ds(pl.multiple_of(seq * piece_rows, piece_rows), piece_rows), wo_cols((mine_there, theirs_there)[i], side)
            ],
            piece_at(side, head, seq),
            z_send.at[side, i],
            z_recv.at[side, i],
            at(buddy, h),
        )
        for i, h in enumerate((head, other))
        for side in range(2)
    ]
    wo_first, wo_second = wo_far[:2], wo_far[2:]

    @pl.when(first)
    def _():
        for copy in wo_first:
            copy.start()

    @pl.when(jnp.logical_not(first))
    def _():
        for copy in wo_second:
            copy.start()

    weight_loads[0].wait()
    weight_loads[1].wait()

    def chunk_at(ref, owner, c):
        return ref.at[pl.ds(owner * blocks_dev + c * chunk_blocks, chunk_blocks)]

    ring = n_seq == 4
    if ring:
        sx, sy = lax.rem(seq, 2), seq // 2
        beside = sy * 2 + (1 - sx)
        across = (1 - sy) * 2 + sx
        peers = [beside, across]
    else:
        peers = [lax.rem(seq + d, n_seq) for d in range(1, n_seq)]

    def kv_copy(kind, peer_at, c):
        ref = (k_all, v_all)[kind]
        return remote(
            chunk_at(ref, seq, c),
            chunk_at(ref, seq, c),
            kv_send.at[kind, peer_at, c],
            kv_recv.at[kind, peer_at, c],
            at_seq(peers[peer_at]),
        )

    def kv_start_early(c):
        if ring:
            kv_copy(0, 1, c).start()
            kv_copy(1, 0, c).start()
        else:
            for p in range(len(peers)):
                kv_copy(0, p, c).start()
                kv_copy(1, p, c).start()

    def kv_start_late():
        if ring:
            for c in range(CHUNKS):
                kv_copy(1, 1, c).start()
                kv_copy(0, 0, c).start()

    for c in range(CHUNKS):
        image_loads[c].wait()
        if c == CHUNKS // 2:
            weight_loads[2].start()
            for load in text_loads:
                load.start()
        both = jnp.dot(
            image[c * chunk_rows : (c + 1) * chunk_rows, :], wkv[...], preferred_element_type=jnp.float32
        ).astype(jnp.bfloat16)
        base = pl.ds(seq * blocks_dev + c * chunk_blocks, chunk_blocks)
        k_all[base] = both[:, :width].reshape(chunk_blocks, BLOCK, width)
        v_all[base] = both[:, width:].reshape(chunk_blocks, BLOCK, width)

        @pl.when(first)
        def _():
            kv_start_early(c)

    @pl.when(first)
    def _():
        kv_start_late()

    for copy in wo_own + wo_near:
        copy.start()

    weight_loads[2].wait()
    for load in text_loads:
        load.wait()

    def query_step(i, carry):
        part = pl.ds(pl.multiple_of(i * text_rows, text_rows), text_rows)
        as_float = text[part, :].astype(jnp.float32)
        inverse = lax.rsqrt(jnp.mean(as_float * as_float, axis=-1, keepdims=True) + EPSILON)
        normed = (as_float * inverse * gain_ref[...]).astype(jnp.bfloat16)
        queries = jnp.dot(normed, wq[...], preferred_element_type=jnp.float32).astype(jnp.bfloat16)
        for u in range(text_rows // TILE):
            for h in range(heads):
                q_all[i * (text_rows // TILE) + u, h * TILE : (h + 1) * TILE, :] = queries[
                    u * TILE : (u + 1) * TILE, h * HEAD_DIM : (h + 1) * HEAD_DIM
                ]
        return carry

    lax.fori_loop(0, text_step, query_step, 0)

    @pl.when(first)
    def _():
        for copy in wo_first:
            copy.wait_send()
        for copy in wo_second:
            copy.start()

    @pl.when(jnp.logical_not(first))
    def _():
        for copy in wo_second:
            copy.wait_send()
        for copy in wo_first:
            copy.start()

    def kv_arrival(kind, peer_at, c):
        ref = (k_all, v_all)[kind]
        back = peer_at if ring else len(peers) - 1 - peer_at
        there = chunk_at(ref, peers[back], c)
        return remote(there, there, kv_send.at[kind, peer_at, c], kv_recv.at[kind, peer_at, c], at_seq(peers[peer_at]))

    def kv_forward(kind, c):
        ref = (k_all, v_all)[kind]
        came, goes = ((across, beside), (beside, across))[kind]
        there = chunk_at(ref, came, c)
        return remote(there, there, fwd_send.at[kind, c], fwd_recv.at[kind, c], at_seq(goes))

    def kv_forwarded(kind, c):
        ref = (k_all, v_all)[kind]
        there = chunk_at(ref, 3 - seq, c)
        return remote(there, there, fwd_send.at[kind, c], fwd_recv.at[kind, c], at_seq(seq))

    @pl.when(jnp.logical_not(first))
    def _():
        pl.semaphore_wait(go_sem, 1)
        for c in range(CHUNKS):
            kv_start_early(c)
        kv_start_late()

    def kv_done(c):
        if ring:
            kv_arrival(0, 0, c).wait_recv()
            kv_arrival(1, 1, c).wait_recv()
            kv_forwarded(0, c).wait_recv()
            kv_forwarded(1, c).wait_recv()
        else:
            for p in range(len(peers)):
                kv_arrival(0, p, c).wait_recv()
                kv_arrival(1, p, c).wait_recv()

    def g_copy(side, i, peer_at):
        piece = piece_at(side, (head, other)[i], seq)
        return remote(piece, piece, g_send.at[side, i, peer_at], g_recv.at[side, i, peer_at], at_seq(peers[peer_at]))

    def g_arrival(side, i, peer_at):
        back = peer_at if ring else len(peers) - 1 - peer_at
        there = piece_at(side, (head, other)[i], peers[back])
        return remote(there, there, g_send.at[side, i, peer_at], g_recv.at[side, i, peer_at], at_seq(peers[peer_at]))

    def g_forward(side, i):
        came, goes = ((across, beside), (beside, across))[i]
        there = piece_at(side, (head, other)[i], came)
        return remote(there, there, gf_send.at[side, i], gf_recv.at[side, i], at_seq(goes))

    def g_forwarded(side, i):
        there = piece_at(side, (head, other)[i], 3 - seq)
        return remote(there, there, gf_send.at[side, i], gf_recv.at[side, i], at_seq(peers[0]))

    def spread_wo(side):
        for i in range(2):
            there = piece_at(side, (head, other)[i], seq)
            remote(there, there, z_send.at[side, i], z_recv.at[side, i], at(buddy, head)).wait_recv()
        for i in range(2):
            if ring:
                g_copy(side, i, 1 - i).start()
            else:
                for p in range(len(peers)):
                    g_copy(side, i, p).start()
        if ring:
            for i in range(2):
                g_copy(side, i, i).start()

    def forward_wo(side):
        if ring:
            for i in range(2):
                g_arrival(side, i, 1 - i).wait_recv()
                g_forward(side, i).start()

    def wo_arrived(side):
        wo_own[side].wait()
        there = wo_all.at[side, slot(0, other)]
        remote(there, there, wo_send.at[side], wo_recv.at[side], at(sec, other)).wait_recv()
        for i in range(2):
            if ring:
                g_arrival(side, i, i).wait_recv()
                g_forwarded(side, i).wait_recv()
            else:
                for p in range(len(peers)):
                    g_arrival(side, i, p).wait_recv()

    if ring:
        for c in range(CHUNKS):
            kv_arrival(0, 1, c).wait_recv()
            kv_forward(0, c).start()
            kv_arrival(1, 0, c).wait_recv()
            kv_forward(1, c).start()

    for c in range(CHUNKS - 1):
        kv_done(c)

    @pl.when(first)
    def _():
        pl.semaphore_signal(go_sem, inc=1, device_id=at(sec, other), device_id_type=MESH)

    kv_done(CHUNKS - 1)

    @pl.when(first)
    def _():
        for side in range(2):
            spread_wo(side)

    def own_copies(t):
        tile = att.at[slot(0, head), t]
        return (
            remote(tile, att.at[slot(1, head), t], a_send.at[0, t], r_pair.at[t], at(buddy, head)),
            remote(tile, tile, a_send.at[1, t], r_core.at[0, t], at(sec, other)),
        )

    def pair_forward(t):
        tile = att.at[slot(1, head), t]
        return remote(tile, tile, a_core.at[t], r_core.at[1, t], at(sec, other))

    def part_copy(side, t):
        return remote(
            part_out.at[side, t], part_in.at[side, t], p_send.at[side, t], p_recv.at[side, t], at(far, other)
        )

    def final_copy(t):
        return remote(part_out.at[0, t], part_in.at[0, t], f_send.at[t], f_recv.at[t], at(sec, other))

    def attend(t):
        for j in range(topk):
            block = sel_ref[t, j]
            k_sel[j * BLOCK : (j + 1) * BLOCK, :] = k_all[block]
            v_sel[j * BLOCK : (j + 1) * BLOCK, :] = v_all[block]
        for h in range(heads):
            kv = (h // group) * HEAD_DIM
            scores = lax.dot_general(
                q_all[t, h * TILE : (h + 1) * TILE, :],
                k_sel[:, kv : kv + HEAD_DIM],
                (((1,), (1,)), ((), ())),
                preferred_element_type=jnp.float32,
            ) * HEAD_DIM ** (-0.5)
            exponent = jnp.exp(scores - jnp.max(scores, axis=-1, keepdims=True))
            weights = (exponent * (1.0 / jnp.sum(exponent, axis=-1, keepdims=True))).astype(jnp.bfloat16)
            att[slot(0, head), t, :, h * HEAD_DIM : (h + 1) * HEAD_DIM] = jnp.dot(
                weights, v_sel[:, kv : kv + HEAD_DIM], preferred_element_type=jnp.float32
            ).astype(jnp.bfloat16)

    def product(side, t):
        total = None
        for i in range(2 * n_head):
            term = jnp.dot(att[i, t], wo_all[side, i], preferred_element_type=jnp.float32)
            total = term if total is None else total + term
        return total

    second = jnp.logical_not(first)
    at_forward = tiles // 2
    lag = jnp.where(first, tiles + 1, tiles)

    def step(s, carry):
        @pl.when(s < tiles)
        def _():
            attend(s)
            for copy in own_copies(s):
                copy.start()

        @pl.when((s >= 1) & (s < tiles + 1))
        def _():
            t = s - 1
            there = att.at[slot(1, head), t]
            remote(there, there, a_send.at[0, t], r_pair.at[t], at(buddy, head)).wait_recv()
            pair_forward(t).start()

        @pl.when(second & (s == 1))
        def _():
            for side in range(2):
                spread_wo(side)

        @pl.when(s == at_forward)
        def _():
            for side in range(2):
                forward_wo(side)

        @pl.when(s == lag)
        def _():
            for side in range(2):
                wo_arrived(side)

        @pl.when((s >= lag) & (s < tiles + lag))
        def _():
            t = s - lag
            rows = pl.ds(pl.multiple_of(t * TILE, TILE), TILE)
            for flag in range(2):
                there = att.at[slot(flag, other), t]
                remote(there, there, a_send.at[1, t], r_core.at[flag, t], at(sec, other)).wait_recv()

            @pl.when(first)
            def _():
                for side in range(2):
                    part_out[side, t] = product(side, t).astype(jnp.bfloat16)
                    part_copy(side, t).start()

            @pl.when(second)
            def _():
                for side in range(2):
                    own = product(side, t)
                    part_copy(side, t).wait_recv()
                    total = (own + part_in[side, t].astype(jnp.float32)).astype(jnp.bfloat16)
                    if side == 0:
                        part_out[0, t] = total
                        final_copy(t).start()
                    else:
                        out_ref[rows, :] = total

        return carry

    lax.fori_loop(0, 2 * tiles + 1, step, 0)

    def take(t, carry):
        final_copy(t).wait_recv()
        out_ref[pl.ds(pl.multiple_of(t * TILE, TILE), TILE), :] = part_in[0, t]
        return carry

    @pl.when(first)
    def _():
        lax.fori_loop(0, tiles, take, 0)

    @pl.when(first)
    def _():
        for copy in wo_second:
            copy.wait_send()

    @pl.when(second)
    def _():
        for copy in wo_first:
            copy.wait_send()

    for copy in wo_near:
        copy.wait_send()
    for side in range(2):
        for i in range(2):
            for p in range(len(peers)):
                g_copy(side, i, p).wait_send()
            if ring:
                g_forward(side, i).wait_send()
    for c in range(CHUNKS):
        for kind in range(2):
            for p in range(len(peers)):
                kv_copy(kind, p, c).wait_send()
            if ring:
                kv_forward(kind, c).wait_send()

    def drain(t, carry):
        for copy in own_copies(t) + (pair_forward(t),):
            copy.wait_send()

        @pl.when(first)
        def _():
            for side in range(2):
                part_copy(side, t).wait_send()

        @pl.when(second)
        def _():
            final_copy(t).wait_send()

        return carry

    lax.fori_loop(0, tiles, drain, 0)


def solution(mesh):
    n_sec, n_seq, n_head = mesh.shape["section"], mesh.shape["seq"], mesh.shape["head"]

    def shards(text, gain, image, wq, wk, wv, wo, selected):
        rows, depth = text.shape
        tiles = rows // TILE
        cols_q = wq.shape[1]
        width = wk.shape[1]
        group = n_sec * n_head
        out_cols = wo.shape[1] // group
        blocks = image.shape[0] // BLOCK * n_seq
        keys = selected.shape[1] * BLOCK
        text_step = max(1, rows // (2 * TILE))
        peers = 2 if n_seq == 4 else n_seq - 1
        bf16 = jnp.bfloat16
        dma = pltpu.SemaphoreType.DMA
        hbm = pl.BlockSpec(memory_space=pl.ANY)
        vmem = pl.BlockSpec(memory_space=pltpu.VMEM)
        return pl.pallas_call(
            functools.partial(kernel, (n_sec, n_seq, n_head)),
            out_shape=jax.ShapeDtypeStruct((rows, out_cols), bf16),
            in_specs=[hbm, vmem, hbm, hbm, hbm, hbm, hbm, pl.BlockSpec(memory_space=pltpu.SMEM)],
            out_specs=vmem,
            scratch_shapes=[
                pltpu.VMEM(text.shape, bf16),
                pltpu.VMEM(image.shape, bf16),
                pltpu.VMEM(wq.shape, bf16),
                pltpu.VMEM((wk.shape[0], 2 * width), bf16),
                pltpu.VMEM((2, 2 * n_head, wo.shape[0], out_cols), bf16),
                pltpu.VMEM((2, tiles, TILE, out_cols), bf16),
                pltpu.VMEM((2, tiles, TILE, out_cols), bf16),
                pltpu.VMEM((blocks, BLOCK, width), bf16),
                pltpu.VMEM((blocks, BLOCK, width), bf16),
                pltpu.VMEM((tiles, cols_q // HEAD_DIM * TILE, HEAD_DIM), bf16),
                pltpu.VMEM((keys, width), bf16),
                pltpu.VMEM((keys, width), bf16),
                pltpu.VMEM((2 * n_head, tiles, TILE, cols_q), bf16),
                dma((text_step,)),
                dma((CHUNKS,)),
                dma((3,)),
                dma((2, peers, CHUNKS)),
                dma((2, peers, CHUNKS)),
                dma((2, CHUNKS)),
                dma((2, CHUNKS)),
                dma((2,)),
                dma((2,)),
                dma((2,)),
                dma((2, 2)),
                dma((2, 2)),
                dma((2, 2, peers)),
                dma((2, 2, peers)),
                dma((2, 2)),
                dma((2, 2)),
                pltpu.SemaphoreType.REGULAR,
                dma((2, tiles)),
                dma((tiles,)),
                dma((tiles,)),
                dma((2, tiles)),
                dma((2, tiles)),
                dma((2, tiles)),
                dma((tiles,)),
                dma((tiles,)),
            ],
            compiler_params=pltpu.CompilerParams(
                collective_id=0, has_side_effects=True, vmem_limit_bytes=60 * 1024 * 1024
            ),
        )(text, gain.reshape(1, depth), image, wq, wk, wv, wo, selected)

    in_specs = (
        P("seq", None),
        P(),
        P("seq", None),
        P(None, ("section", "head")),
        P(None, ("section", "head")),
        P(None, ("section", "head")),
        P(("section", "head"), None),
        P("seq", None),
    )
    out_specs = P("seq", ("section", "head"))
    return jax.shard_map(shards, mesh=mesh, in_specs=in_specs, out_specs=out_specs, check_vma=False)
```

```python
import functools

import jax
import jax.numpy as jnp
from jax import lax
from jax.experimental import pallas as pl
from jax.experimental.pallas import tpu as pltpu
from jax.sharding import PartitionSpec as P

HEAD_DIM = 128
TILE = 128
BLOCK = 64
EPSILON = 1e-05
CHUNKS = 4
MESH = pl.DeviceIdType.MESH


def kernel(
    sizes,
    text_hbm,
    gain_ref,
    image_hbm,
    wq_hbm,
    wk_hbm,
    wv_hbm,
    wo_hbm,
    sel_ref,
    out_ref,
    text,
    image,
    wq,
    wkv,
    wo_all,
    part_out,
    part_in,
    k_all,
    v_all,
    q_all,
    k_sel,
    v_sel,
    att,
    text_sem,
    image_sem,
    weight_sem,
    kv_send,
    kv_recv,
    fwd_send,
    fwd_recv,
    wo_local,
    wo_send,
    wo_recv,
    z_send,
    z_recv,
    g_send,
    g_recv,
    gf_send,
    gf_recv,
    go_sem,
    a_send,
    a_core,
    r_pair,
    r_core,
    p_send,
    p_recv,
    f_send,
    f_recv,
):
    n_sec, n_seq, n_head = sizes
    sec = lax.axis_index("section")
    seq = lax.axis_index("seq")
    head = lax.axis_index("head")
    tiles = q_all.shape[0]
    qk_rows = q_all.shape[1]
    heads = qk_rows // TILE
    width = k_all.shape[-1]
    local_kv = width // HEAD_DIM
    group = heads // local_kv
    topk = sel_ref.shape[1]
    rows_img = image.shape[0]
    blocks_dev = rows_img // BLOCK
    chunk_blocks = blocks_dev // CHUNKS
    chunk_rows = chunk_blocks * BLOCK
    out_cols = out_ref.shape[1]
    text_step = text_sem.shape[0]
    text_rows = text.shape[0] // text_step

    other = 1 - head
    buddy = lax.rem(sec + n_sec // 2, n_sec)
    far = sec + 1 - 2 * lax.rem(sec, 2)
    buddy_far = buddy + 1 - 2 * lax.rem(buddy, 2)
    first = head == 0
    mine, theirs = jnp.where(first, far, sec), jnp.where(first, sec, far)
    mine_there, theirs_there = jnp.where(first, buddy_far, buddy), jnp.where(first, buddy, buddy_far)

    def at(s, h):
        return {"section": s, "seq": seq, "head": h}

    def at_seq(q):
        return {"section": sec, "seq": q, "head": head}

    def remote(src, dst, send, recv, device):
        return pltpu.make_async_remote_copy(
            src_ref=src, dst_ref=dst, send_sem=send, recv_sem=recv, device_id=device, device_id_type=MESH
        )

    weight_loads = [
        pltpu.make_async_copy(wk_hbm, wkv.at[:, pl.ds(0, width)], weight_sem.at[0]),
        pltpu.make_async_copy(wv_hbm, wkv.at[:, pl.ds(width, width)], weight_sem.at[1]),
        pltpu.make_async_copy(wq_hbm, wq, weight_sem.at[2]),
    ]
    image_loads = [
        pltpu.make_async_copy(
            image_hbm.at[pl.ds(c * chunk_rows, chunk_rows)],
            image.at[pl.ds(c * chunk_rows, chunk_rows)],
            image_sem.at[c],
        )
        for c in range(CHUNKS)
    ]
    text_loads = [
        pltpu.make_async_copy(
            text_hbm.at[pl.ds(c * text_rows, text_rows)],
            text.at[pl.ds(c * text_rows, text_rows)],
            text_sem.at[c],
        )
        for c in range(text_step)
    ]
    weight_loads[0].start()
    weight_loads[1].start()
    for load in image_loads:
        load.start()

    barrier = pltpu.get_barrier_semaphore()
    for d in range(1, n_seq):
        pl.semaphore_signal(barrier, inc=1, device_id=at_seq(lax.rem(seq + d, n_seq)), device_id_type=MESH)
    for d in range(n_sec):
        for e in range(n_head):
            if d or e:
                pl.semaphore_signal(
                    barrier,
                    inc=1,
                    device_id=at(lax.rem(sec + d, n_sec), lax.rem(head + e, n_head)),
                    device_id_type=MESH,
                )
    pl.semaphore_wait(barrier, n_seq - 1 + n_sec * n_head - 1)

    def slot(flag, h):
        return flag * n_head + h

    def wo_cols(s, h):
        return pl.ds(pl.multiple_of((s * n_head + h) * out_cols, out_cols), out_cols)

    wo_own = [
        pltpu.make_async_copy(
            wo_hbm.at[:, wo_cols(mine, side)], wo_all.at[side, slot(0, head)], wo_local.at[side]
        )
        for side in range(2)
    ]
    wo_near = [
        remote(
            wo_hbm.at[:, wo_cols(theirs, side)],
            wo_all.at[side, slot(0, head)],
            wo_send.at[side],
            wo_recv.at[side],
            at(sec, other),
        )
        for side in range(2)
    ]
    piece_rows = wo_hbm.shape[0] // n_seq

    def piece_at(side, h, owner):
        return wo_all.at[side, slot(1, h), pl.ds(pl.multiple_of(owner * piece_rows, piece_rows), piece_rows)]

    wo_far = [
        remote(
            wo_hbm.at[
                pl.ds(pl.multiple_of(seq * piece_rows, piece_rows), piece_rows), wo_cols((mine_there, theirs_there)[i], side)
            ],
            piece_at(side, head, seq),
            z_send.at[side, i],
            z_recv.at[side, i],
            at(buddy, h),
        )
        for i, h in enumerate((head, other))
        for side in range(2)
    ]
    wo_first, wo_second = wo_far[:2], wo_far[2:]

    @pl.when(first)
    def _():
        for copy in wo_first:
            copy.start()

    @pl.when(jnp.logical_not(first))
    def _():
        for copy in wo_second:
            copy.start()

    weight_loads[0].wait()
    weight_loads[1].wait()

    def chunk_at(ref, owner, c):
        return ref.at[pl.ds(owner * blocks_dev + c * chunk_blocks, chunk_blocks)]

    ring = n_seq == 4
    if ring:
        sx, sy = lax.rem(seq, 2), seq // 2
        beside = sy * 2 + (1 - sx)
        across = (1 - sy) * 2 + sx
        peers = [beside, across]
    else:
        peers = [lax.rem(seq + d, n_seq) for d in range(1, n_seq)]

    def kv_copy(kind, peer_at, c):
        ref = (k_all, v_all)[kind]
        return remote(
            chunk_at(ref, seq, c),
            chunk_at(ref, seq, c),
            kv_send.at[kind, peer_at, c],
            kv_recv.at[kind, peer_at, c],
            at_seq(peers[peer_at]),
        )

    def kv_start_early(c):
        if ring:
            kv_copy(0, 1, c).start()
            kv_copy(1, 0, c).start()
        else:
            for p in range(len(peers)):
                kv_copy(0, p, c).start()
                kv_copy(1, p, c).start()

    def kv_start_late():
        if ring:
            for c in range(CHUNKS):
                kv_copy(1, 1, c).start()
                kv_copy(0, 0, c).start()

    for c in range(CHUNKS):
        image_loads[c].wait()
        if c == CHUNKS // 2:
            weight_loads[2].start()
            for load in text_loads:
                load.start()
        both = jnp.dot(
            image[c * chunk_rows : (c + 1) * chunk_rows, :], wkv[...], preferred_element_type=jnp.float32
        ).astype(jnp.bfloat16)
        base = pl.ds(seq * blocks_dev + c * chunk_blocks, chunk_blocks)
        k_all[base] = both[:, :width].reshape(chunk_blocks, BLOCK, width)
        v_all[base] = both[:, width:].reshape(chunk_blocks, BLOCK, width)

        @pl.when(first)
        def _():
            kv_start_early(c)

    @pl.when(first)
    def _():
        kv_start_late()

    for copy in wo_own + wo_near:
        copy.start()

    weight_loads[2].wait()
    for load in text_loads:
        load.wait()

    def kv_arrival(kind, peer_at, c):
        ref = (k_all, v_all)[kind]
        back = peer_at if ring else len(peers) - 1 - peer_at
        there = chunk_at(ref, peers[back], c)
        return remote(there, there, kv_send.at[kind, peer_at, c], kv_recv.at[kind, peer_at, c], at_seq(peers[peer_at]))

    def kv_forward(kind, c):
        ref = (k_all, v_all)[kind]
        came, goes = ((across, beside), (beside, across))[kind]
        there = chunk_at(ref, came, c)
        return remote(there, there, fwd_send.at[kind, c], fwd_recv.at[kind, c], at_seq(goes))

    def kv_forwarded(kind, c):
        ref = (k_all, v_all)[kind]
        there = chunk_at(ref, 3 - seq, c)
        return remote(there, there, fwd_send.at[kind, c], fwd_recv.at[kind, c], at_seq(seq))

    def forward_kv(c):
        kv_arrival(0, 1, c).wait_recv()
        kv_forward(0, c).start()
        kv_arrival(1, 0, c).wait_recv()
        kv_forward(1, c).start()

    def query_step(i, carry):
        part = pl.ds(pl.multiple_of(i * text_rows, text_rows), text_rows)
        as_float = text[part, :].astype(jnp.float32)
        inverse = lax.rsqrt(jnp.mean(as_float * as_float, axis=-1, keepdims=True) + EPSILON)
        normed = (as_float * inverse * gain_ref[...]).astype(jnp.bfloat16)
        queries = jnp.dot(normed, wq[...], preferred_element_type=jnp.float32).astype(jnp.bfloat16)
        for u in range(text_rows // TILE):
            for h in range(heads):
                q_all[i * (text_rows // TILE) + u, h * TILE : (h + 1) * TILE, :] = queries[
                    u * TILE : (u + 1) * TILE, h * HEAD_DIM : (h + 1) * HEAD_DIM
                ]
        if ring:
            for c in range(CHUNKS):

                @pl.when(first & (i == min(c, text_step - 1)))
                def _():
                    forward_kv(c)

        return carry

    lax.fori_loop(0, text_step, query_step, 0)

    @pl.when(first)
    def _():
        for copy in wo_first:
            copy.wait_send()
        for copy in wo_second:
            copy.start()

    @pl.when(jnp.logical_not(first))
    def _():
        for copy in wo_second:
            copy.wait_send()
        for copy in wo_first:
            copy.start()

    @pl.when(jnp.logical_not(first))
    def _():
        pl.semaphore_wait(go_sem, 1)
        for c in range(CHUNKS):
            kv_start_early(c)
        kv_start_late()

    def kv_done(c):
        if ring:
            kv_arrival(0, 0, c).wait_recv()
            kv_arrival(1, 1, c).wait_recv()
            kv_forwarded(0, c).wait_recv()
            kv_forwarded(1, c).wait_recv()
        else:
            for p in range(len(peers)):
                kv_arrival(0, p, c).wait_recv()
                kv_arrival(1, p, c).wait_recv()

    def g_copy(side, i, peer_at):
        piece = piece_at(side, (head, other)[i], seq)
        return remote(piece, piece, g_send.at[side, i, peer_at], g_recv.at[side, i, peer_at], at_seq(peers[peer_at]))

    def g_arrival(side, i, peer_at):
        back = peer_at if ring else len(peers) - 1 - peer_at
        there = piece_at(side, (head, other)[i], peers[back])
        return remote(there, there, g_send.at[side, i, peer_at], g_recv.at[side, i, peer_at], at_seq(peers[peer_at]))

    def g_forward(side, i):
        came, goes = ((across, beside), (beside, across))[i]
        there = piece_at(side, (head, other)[i], came)
        return remote(there, there, gf_send.at[side, i], gf_recv.at[side, i], at_seq(goes))

    def g_forwarded(side, i):
        there = piece_at(side, (head, other)[i], 3 - seq)
        return remote(there, there, gf_send.at[side, i], gf_recv.at[side, i], at_seq(peers[0]))

    def spread_wo(side):
        for i in range(2):
            there = piece_at(side, (head, other)[i], seq)
            remote(there, there, z_send.at[side, i], z_recv.at[side, i], at(buddy, head)).wait_recv()
        for i in range(2):
            if ring:
                g_copy(side, i, 1 - i).start()
            else:
                for p in range(len(peers)):
                    g_copy(side, i, p).start()
        if ring:
            for i in range(2):
                g_copy(side, i, i).start()

    def forward_wo(side):
        if ring:
            for i in range(2):
                g_arrival(side, i, 1 - i).wait_recv()
                g_forward(side, i).start()

    def wo_arrived(side):
        wo_own[side].wait()
        there = wo_all.at[side, slot(0, other)]
        remote(there, there, wo_send.at[side], wo_recv.at[side], at(sec, other)).wait_recv()
        for i in range(2):
            if ring:
                g_arrival(side, i, i).wait_recv()
                g_forwarded(side, i).wait_recv()
            else:
                for p in range(len(peers)):
                    g_arrival(side, i, p).wait_recv()

    @pl.when(jnp.logical_not(first))
    def _():
        if ring:
            for c in range(CHUNKS):
                forward_kv(c)

    for c in range(CHUNKS - 1):
        kv_done(c)

    @pl.when(first)
    def _():
        pl.semaphore_signal(go_sem, inc=1, device_id=at(sec, other), device_id_type=MESH)

    kv_done(CHUNKS - 1)

    def own_copies(t):
        tile = att.at[slot(0, head), t]
        return (
            remote(tile, att.at[slot(1, head), t], a_send.at[0, t], r_pair.at[t], at(buddy, head)),
            remote(tile, tile, a_send.at[1, t], r_core.at[0, t], at(sec, other)),
        )

    def pair_forward(t):
        tile = att.at[slot(1, head), t]
        return remote(tile, tile, a_core.at[t], r_core.at[1, t], at(sec, other))

    def part_copy(side, t):
        return remote(
            part_out.at[side, t], part_in.at[side, t], p_send.at[side, t], p_recv.at[side, t], at(far, other)
        )

    def final_copy(t):
        return remote(part_out.at[0, t], part_in.at[0, t], f_send.at[t], f_recv.at[t], at(sec, other))

    def attend(t):
        for j in range(topk):
            block = sel_ref[t, j]
            k_sel[j * BLOCK : (j + 1) * BLOCK, :] = k_all[block]
            v_sel[j * BLOCK : (j + 1) * BLOCK, :] = v_all[block]
        for h in range(heads):
            kv = (h // group) * HEAD_DIM
            scores = lax.dot_general(
                q_all[t, h * TILE : (h + 1) * TILE, :],
                k_sel[:, kv : kv + HEAD_DIM],
                (((1,), (1,)), ((), ())),
                preferred_element_type=jnp.float32,
            ) * HEAD_DIM ** (-0.5)
            exponent = jnp.exp(scores - jnp.max(scores, axis=-1, keepdims=True))
            weights = (exponent * (1.0 / jnp.sum(exponent, axis=-1, keepdims=True))).astype(jnp.bfloat16)
            att[slot(0, head), t, :, h * HEAD_DIM : (h + 1) * HEAD_DIM] = jnp.dot(
                weights, v_sel[:, kv : kv + HEAD_DIM], preferred_element_type=jnp.float32
            ).astype(jnp.bfloat16)

    def product(side, t):
        total = None
        for i in range(2 * n_head):
            term = jnp.dot(att[i, t], wo_all[side, i], preferred_element_type=jnp.float32)
            total = term if total is None else total + term
        return total

    second = jnp.logical_not(first)
    at_spread = jnp.where(first, tiles // 4, 1)
    at_forward = jnp.where(first, 3 * tiles // 4, 3 * tiles // 8)
    lag = jnp.where(first, tiles + 1, tiles)

    def step(s, carry):
        @pl.when(s < tiles)
        def _():
            attend(s)
            for copy in own_copies(s):
                copy.start()

        @pl.when((s >= 1) & (s < tiles + 1))
        def _():
            t = s - 1
            there = att.at[slot(1, head), t]
            remote(there, there, a_send.at[0, t], r_pair.at[t], at(buddy, head)).wait_recv()
            pair_forward(t).start()

        @pl.when(s == at_spread)
        def _():
            for side in range(2):
                spread_wo(side)

        @pl.when(s == at_forward)
        def _():
            for side in range(2):
                forward_wo(side)

        @pl.when(s == lag)
        def _():
            for side in range(2):
                wo_arrived(side)

        @pl.when((s >= lag) & (s < tiles + lag))
        def _():
            t = s - lag
            rows = pl.ds(pl.multiple_of(t * TILE, TILE), TILE)
            for flag in range(2):
                there = att.at[slot(flag, other), t]
                remote(there, there, a_send.at[1, t], r_core.at[flag, t], at(sec, other)).wait_recv()

            @pl.when(first)
            def _():
                for side in range(2):
                    part_out[side, t] = product(side, t).astype(jnp.bfloat16)
                    part_copy(side, t).start()

            @pl.when(second)
            def _():
                for side in range(2):
                    own = product(side, t)
                    part_copy(side, t).wait_recv()
                    total = (own + part_in[side, t].astype(jnp.float32)).astype(jnp.bfloat16)
                    if side == 0:
                        part_out[0, t] = total
                        final_copy(t).start()
                    else:
                        out_ref[rows, :] = total

        return carry

    lax.fori_loop(0, 2 * tiles + 1, step, 0)

    def take(t, carry):
        final_copy(t).wait_recv()
        out_ref[pl.ds(pl.multiple_of(t * TILE, TILE), TILE), :] = part_in[0, t]
        return carry

    @pl.when(first)
    def _():
        lax.fori_loop(0, tiles, take, 0)

    @pl.when(first)
    def _():
        for copy in wo_second:
            copy.wait_send()

    @pl.when(second)
    def _():
        for copy in wo_first:
            copy.wait_send()

    for copy in wo_near:
        copy.wait_send()
    for side in range(2):
        for i in range(2):
            for p in range(len(peers)):
                g_copy(side, i, p).wait_send()
            if ring:
                g_forward(side, i).wait_send()
    for c in range(CHUNKS):
        for kind in range(2):
            for p in range(len(peers)):
                kv_copy(kind, p, c).wait_send()
            if ring:
                kv_forward(kind, c).wait_send()

    def drain(t, carry):
        for copy in own_copies(t) + (pair_forward(t),):
            copy.wait_send()

        @pl.when(first)
        def _():
            for side in range(2):
                part_copy(side, t).wait_send()

        @pl.when(second)
        def _():
            final_copy(t).wait_send()

        return carry

    lax.fori_loop(0, tiles, drain, 0)


def solution(mesh):
    n_sec, n_seq, n_head = mesh.shape["section"], mesh.shape["seq"], mesh.shape["head"]

    def shards(text, gain, image, wq, wk, wv, wo, selected):
        rows, depth = text.shape
        tiles = rows // TILE
        cols_q = wq.shape[1]
        width = wk.shape[1]
        group = n_sec * n_head
        out_cols = wo.shape[1] // group
        blocks = image.shape[0] // BLOCK * n_seq
        keys = selected.shape[1] * BLOCK
        text_step = max(1, rows // (2 * TILE))
        peers = 2 if n_seq == 4 else n_seq - 1
        bf16 = jnp.bfloat16
        dma = pltpu.SemaphoreType.DMA
        hbm = pl.BlockSpec(memory_space=pl.ANY)
        vmem = pl.BlockSpec(memory_space=pltpu.VMEM)
        return pl.pallas_call(
            functools.partial(kernel, (n_sec, n_seq, n_head)),
            out_shape=jax.ShapeDtypeStruct((rows, out_cols), bf16),
            in_specs=[hbm, vmem, hbm, hbm, hbm, hbm, hbm, pl.BlockSpec(memory_space=pltpu.SMEM)],
            out_specs=vmem,
            scratch_shapes=[
                pltpu.VMEM(text.shape, bf16),
                pltpu.VMEM(image.shape, bf16),
                pltpu.VMEM(wq.shape, bf16),
                pltpu.VMEM((wk.shape[0], 2 * width), bf16),
                pltpu.VMEM((2, 2 * n_head, wo.shape[0], out_cols), bf16),
                pltpu.VMEM((2, tiles, TILE, out_cols), bf16),
                pltpu.VMEM((2, tiles, TILE, out_cols), bf16),
                pltpu.VMEM((blocks, BLOCK, width), bf16),
                pltpu.VMEM((blocks, BLOCK, width), bf16),
                pltpu.VMEM((tiles, cols_q // HEAD_DIM * TILE, HEAD_DIM), bf16),
                pltpu.VMEM((keys, width), bf16),
                pltpu.VMEM((keys, width), bf16),
                pltpu.VMEM((2 * n_head, tiles, TILE, cols_q), bf16),
                dma((text_step,)),
                dma((CHUNKS,)),
                dma((3,)),
                dma((2, peers, CHUNKS)),
                dma((2, peers, CHUNKS)),
                dma((2, CHUNKS)),
                dma((2, CHUNKS)),
                dma((2,)),
                dma((2,)),
                dma((2,)),
                dma((2, 2)),
                dma((2, 2)),
                dma((2, 2, peers)),
                dma((2, 2, peers)),
                dma((2, 2)),
                dma((2, 2)),
                pltpu.SemaphoreType.REGULAR,
                dma((2, tiles)),
                dma((tiles,)),
                dma((tiles,)),
                dma((2, tiles)),
                dma((2, tiles)),
                dma((2, tiles)),
                dma((tiles,)),
                dma((tiles,)),
            ],
            compiler_params=pltpu.CompilerParams(
                collective_id=0, has_side_effects=True, vmem_limit_bytes=60 * 1024 * 1024
            ),
        )(text, gain.reshape(1, depth), image, wq, wk, wv, wo, selected)

    in_specs = (
        P("seq", None),
        P(),
        P("seq", None),
        P(None, ("section", "head")),
        P(None, ("section", "head")),
        P(None, ("section", "head")),
        P(("section", "head"), None),
        P("seq", None),
    )
    out_specs = P("seq", ("section", "head"))
    return jax.shard_map(shards, mesh=mesh, in_specs=in_specs, out_specs=out_specs, check_vma=False)
```
